32 devices in a mesh: groups: 2 (over x), seq: 16 (over z, y, core).
Axes of the slice: x: 2, y: 2, z: 4, core: 2. Of those that a mesh axis runs over, the one named last changes fastest.
Arguments:
- first_queries: bfloat16 [4096, 2048], P(('groups', 'seq')), parts along dimension 0, may hold values from -12 to 12
- second_queries: bfloat16 [4096, 2048], P(('groups', 'seq')), parts along dimension 0, may hold values from -12 to 12
- common_keys: bfloat16 [4096, 512], P(('groups', 'seq')), parts along dimension 0, may hold values from -4 to 4
- common_values: bfloat16 [4096, 512], P(('groups', 'seq')), parts along dimension 0, may hold values from -6 to 6
- lengths: int32 [8], P('groups'), parts along dimension 0, may hold values from 1 to 1024, 2048 in all
Outputs:
- first_output: bfloat16 [4096, 2048], P(('groups', 'seq')), parts along dimension 0
- second_output: bfloat16 [4096, 2048], P(('groups', 'seq')), parts along dimension 0
The draws below stay inside these ranges and needn't reach their ends.
There are 2 independent parts, one for each index of `groups`. The reference program is written for one: setup_inputs(seed, part) draws one part's arguments, and reference() takes and returns one part's arrays. A program takes and returns all parts, laid end to end along the dimension named above; each array names one. Nothing has to cross between parts.
Inputs may be any that keep to these rules, and one draw needn't show every extreme that they name: `lengths`: the 4 documents lie end to end in order and fill all 2048 positions.
All inputs are finite; a program needn't handle non-finite values.
Results may differ from the reference program's by a relative error of at most 0.0034.
Values may be sent and summed in bfloat16 or wider, within the bound.
No kernel may reach another device: no remote copies, remote signals or barrier semaphores. Data moves between devices by JAX's collectives and lax.ppermute only.
A program may use at most 64 MiB of HBM per device.

```python
import math
import jax
import jax.numpy as jnp
import numpy as np
from jax import lax

HEAD_WIDTH = 128
QUERY_HEAD_COUNT = 16
KEY_VALUE_HEADS = 4
NDOC = 4
GROUP_TOKENS = 2048


def query_draw(key, salt_value):
    random_seed_key = jax.random.fold_in(key, salt_value)
    random_jitter = jnp.clip(2.0 * jax.random.normal(random_seed_key, (GROUP_TOKENS, QUERY_HEAD_COUNT * HEAD_WIDTH), jnp.float32), -8.0, 8.0)
    return random_jitter.astype(jnp.bfloat16)


def draw_first_queries(key, part):
    return query_draw(key, 21)


def draw_second_queries(key, part):
    return query_draw(key, 22)


def draw_common_keys(key, part):
    random_seed_key = jax.random.fold_in(key, 31)
    random_jitter = jnp.clip(jax.random.normal(random_seed_key, (GROUP_TOKENS, KEY_VALUE_HEADS * HEAD_WIDTH), jnp.float32), -4.0, 4.0)
    return random_jitter.astype(jnp.bfloat16)


def block_levels(key, shape, split, least, largest):
    def one(dim, parts):
        steps = jax.random.uniform(jax.random.fold_in(jax.random.fold_in(key, 6), dim), (parts,), jnp.float32, least / len(split), largest / len(split))
        return jnp.repeat(jnp.exp(steps), shape[dim] // parts).reshape((-1,) + (1,) * (len(shape) - dim - 1))

    level = one(*split[0])
    for cut in split[1:]:
        level = level * one(*cut)
    return level


def split_up(amount, total, reach, slope):
    loads = [(1 << 20) // math.isqrt(grade ** slope) + 1 for grade in range(2, amount + 1)]
    rest, given = total - reach - (amount - 1), [1] * (amount - 1)
    while rest > 0:
        movable = [i for i in range(amount - 1) if given[i] < reach]
        whole, budget = sum([loads[i] for i in movable]), rest
        for i in movable:
            addition = min(reach - given[i], max(1, budget * loads[i] // whole), rest)
            given[i] = given[i] + addition
            rest = rest - addition
    return np.array([reach] + given)


def ragged_sizes(stream_key, count, total, most, slope):
    if count == 2:
        one = jax.random.randint(stream_key, (), max(1, total - most), min(most, total - 1) + 1)
        return jnp.stack([one, total - one])
    tallies = jnp.asarray(split_up(count, total, most, slope), jnp.int32)
    twos = (count - 1) // 2
    donor, sink = tallies[1:1 + 2 * twos:2], tallies[2:2 + 2 * twos:2]
    margin = jnp.minimum(donor - 1, most - sink)
    passed = jax.random.randint(jax.random.fold_in(stream_key, 1), (twos,), 0, 1 << 20) % (margin + 1)
    tallies = tallies.at[1:1 + 2 * twos:2].set(donor - passed).at[2:2 + 2 * twos:2].set(sink + passed)
    return tallies[jax.random.permutation(jax.random.fold_in(stream_key, 2), count)]


def scatter_about(own_key, shape, spread, most, cuts=(), kind=jnp.bfloat16):
    drawn = spread * jax.random.normal(own_key, shape, jnp.float32)
    if cuts:
        drawn = drawn * block_levels(own_key, shape, cuts, -0.22, 0.18)
    return jnp.clip(drawn, -most, most).astype(kind)


def setup_inputs(seed: int = 0, part: int = 0) -> dict:
    keys = jax.random.split(jax.random.key(seed), 6)
    part_splits = jax.random.split(jax.random.fold_in(keys[5], part), 6)
    return {
        "first_queries": draw_first_queries(jax.random.fold_in(jax.random.fold_in(keys[5], part), 71), part),
        "second_queries": draw_second_queries(jax.random.fold_in(jax.random.fold_in(keys[5], part), 71), part),
        "common_keys": draw_common_keys(jax.random.fold_in(jax.random.fold_in(keys[5], part), 71), part),
        "common_values": scatter_about(part_splits[3], (GROUP_TOKENS, KEY_VALUE_HEADS * HEAD_WIDTH), 1.0, 6.0, ((0, 16),)),
        "lengths": ragged_sizes(part_splits[4], NDOC, GROUP_TOKENS, GROUP_TOKENS // 2, 2).astype(jnp.int32),
    }


def reference(first_queries, second_queries, common_keys, common_values, lengths):
    positions = jnp.arange(GROUP_TOKENS, dtype=jnp.int32)
    bounds = jnp.cumsum(lengths)
    documents = jnp.sum((positions[:, None] >= bounds[None, :-1]).astype(jnp.int32), axis=1)
    visible = (positions[None, :] <= positions[:, None]) & (documents[None, :] == documents[:, None])
    key_head_count = common_keys.astype(jnp.float32).reshape(GROUP_TOKENS, KEY_VALUE_HEADS, HEAD_WIDTH).transpose(1, 0, 2)
    value_head_count = common_values.astype(jnp.float32).reshape(GROUP_TOKENS, KEY_VALUE_HEADS, HEAD_WIDTH).transpose(1, 0, 2)

    def attend_layer(queries):
        query_heads = queries.astype(jnp.float32).reshape(GROUP_TOKENS, QUERY_HEAD_COUNT, HEAD_WIDTH).transpose(1, 0, 2)

        def one_head(head_position):
            query_head = query_heads[head_position]
            shared_tensor = head_position // (QUERY_HEAD_COUNT // KEY_VALUE_HEADS)
            scores = jnp.einsum("qd,kd->qk", query_head, key_head_count[shared_tensor]) * (HEAD_WIDTH ** -0.5)
            masked = jnp.where(visible, scores, -1e30)
            highest = jnp.max(masked, axis=1, keepdims=True)
            weights = jnp.where(visible, jnp.exp(masked - highest), 0.0)
            row_total = jnp.sum(weights, axis=1, keepdims=True)
            rounded = lax.optimization_barrier(weights.astype(jnp.bfloat16)).astype(jnp.float32)
            blended = jnp.einsum("qk,kd->qd", rounded, value_head_count[shared_tensor])
            return (blended / row_total).astype(jnp.bfloat16)

        head_outputs = lax.map(one_head, jnp.arange(QUERY_HEAD_COUNT, dtype=jnp.int32))
        return head_outputs.transpose(1, 0, 2).reshape(GROUP_TOKENS, QUERY_HEAD_COUNT * HEAD_WIDTH)

    return attend_layer(first_queries), attend_layer(second_queries)
```

```python
import functools
import math

import jax
import jax.numpy as jnp
from jax import lax
from jax.experimental import pallas as pl
from jax.experimental.pallas import tpu as pltpu
from jax.sharding import PartitionSpec as P


HEAD_WIDTH = 128
QUERY_HEAD_COUNT = 16
KEY_VALUE_HEADS = 4

CORE = 1
ROW = 2
LEVEL = 4

HIDDEN = -1e30
NOWHERE = -(1 << 20)
PAIR = 2


def swapped(count, distance):
    return [(d, d ^ distance) for d in range(count)]


def shifted(count):
    return [(d, d + LEVEL) for d in range(count - LEVEL)]


def across(count):
    return [(d, d + LEVEL - ROW) for d in range(count - LEVEL) if d & ROW]


def pack_kernel(keys_ref, values_ref, packed_ref):
    for g in range(KEY_VALUE_HEADS):
        columns = pl.ds(g * HEAD_WIDTH, HEAD_WIDTH)
        packed_ref[g] = keys_ref[:, columns]
        packed_ref[KEY_VALUE_HEADS + g] = values_ref[:, columns].T


def pack(keys, values):
    tokens = keys.shape[0]
    return pl.pallas_call(
        pack_kernel,
        out_shape=jax.ShapeDtypeStruct((2 * KEY_VALUE_HEADS, tokens, HEAD_WIDTH), keys.dtype),
        name="pack",
    )(keys, values)


def attend_kernel(sources, count, first, last, *refs):
    refs = list(refs)
    device_ref, lengths_ref, first_ref, second_ref = refs[:4]
    blocks = refs[4 : 4 + count]
    rest = refs[4 + count :]
    if not first:
        sum_in, stat_in = rest[:2]
        rest = rest[2:]
    if last:
        out_refs, rest = rest[:2], rest[2:]
    else:
        sum_ref, stat_ref = rest[:2]
        rest = rest[2:]
    (bias_ref,) = rest
    if first:
        sum_in, stat_in = None, None

    tokens = first_ref.shape[0]
    device = device_ref[0]
    query_base = device * tokens
    bounds = []
    total = 0
    for k in range(lengths_ref.shape[0] - 1):
        total = total + lengths_ref[k]
        bounds.append(total)

    def start_of(place):
        start = jnp.zeros_like(place)
        for bound in bounds:
            start = jnp.where(place >= bound, bound, start)
        return start

    bases = []
    for source in sources:
        bases.append(source(device) * tokens)
    earliest = start_of(query_base)
    needed = functools.reduce(
        jnp.logical_or,
        [(b <= query_base + tokens - 1) & (b + tokens - 1 >= earliest) for b in bases],
    )

    group = QUERY_HEAD_COUNT // KEY_VALUE_HEADS
    pairs = group // PAIR
    steps = [(g, layer, pair) for g in range(KEY_VALUE_HEADS) for layer in range(2) for pair in range(pairs)]
    factor = math.log2(math.e) / math.sqrt(HEAD_WIDTH)

    def scores(step):
        g, layer, pair = step
        source = (first_ref, second_ref)[layer]
        head = g * group + pair * PAIR
        query = jnp.concatenate(
            [source[:, (head + i) * HEAD_WIDTH : (head + i + 1) * HEAD_WIDTH] for i in range(PAIR)], axis=0
        )
        keys = jnp.concatenate([b[g] for b in blocks], axis=0)
        return lax.dot_general(keys, query, (((1,), (1,)), ((), ())), preferred_element_type=jnp.float32)

    def absorb():
        place = query_base + lax.broadcasted_iota(jnp.int32, (1, tokens), 1)
        start = start_of(place)
        for i, base in enumerate(bases):
            key_place = base + lax.broadcasted_iota(jnp.int32, (tokens, tokens), 0)
            visible = (key_place >= start) & (key_place <= place)
            bias = jnp.where(visible, 0.0, HIDDEN)
            for j in range(PAIR):
                bias_ref[i * tokens : (i + 1) * tokens, j * tokens : (j + 1) * tokens] = bias

        ahead = scores(steps[0])
        for n, step in enumerate(steps):
            g, _, _ = step
            raw = ahead
            if n + 1 < len(steps):
                ahead = scores(steps[n + 1])
            masked = raw * factor + bias_ref[...]
            highest = jnp.max(masked, axis=0, keepdims=True)
            if not first:
                former = stat_in[2 * n : 2 * n + 1, :]
                highest = jnp.maximum(highest, former)
            weights = jnp.exp2(masked - highest)
            row_sum = jnp.sum(weights, axis=0, keepdims=True)
            values = jnp.concatenate([b[KEY_VALUE_HEADS + g] for b in blocks], axis=1)
            product = jnp.dot(values, weights.astype(jnp.bfloat16), preferred_element_type=jnp.float32)
            if not first:
                fade = jnp.exp2(former - highest)
                row_sum = row_sum + stat_in[2 * n + 1 : 2 * n + 2, :] * fade
                product = product + sum_in[n] * fade
            finish(n, step, product, row_sum, highest)

    def finish(n, step, product, row_sum, highest):
        g, layer, pair = step
        if last:
            blended = product * (1.0 / row_sum)
            head = g * group + pair * PAIR
            for i in range(PAIR):
                columns = slice((head + i) * HEAD_WIDTH, (head + i + 1) * HEAD_WIDTH)
                out_refs[layer][:, columns] = blended[:, i * tokens : (i + 1) * tokens].T.astype(jnp.bfloat16)
        else:
            sum_ref[n] = product
            stat_ref[2 * n : 2 * n + 1, :] = highest
            stat_ref[2 * n + 1 : 2 * n + 2, :] = row_sum

    if first:
        absorb()
    else:
        pl.when(needed)(absorb)

        @pl.when(jnp.logical_not(needed))
        def _():
            for n, step in enumerate(steps):
                finish(n, step, sum_in[n], stat_in[2 * n + 1 : 2 * n + 2, :], stat_in[2 * n : 2 * n + 1, :])


def attend(device, lengths, first_queries, second_queries, blocks, sources, state, last):
    tokens = first_queries.shape[0]
    steps = 2 * QUERY_HEAD_COUNT // PAIR
    width = PAIR * tokens
    state_shapes = [
        jax.ShapeDtypeStruct((steps, HEAD_WIDTH, width), jnp.float32),
        jax.ShapeDtypeStruct((2 * steps, width), jnp.float32),
    ]
    in_vmem = pl.BlockSpec(memory_space=pltpu.VMEM)
    in_smem = pl.BlockSpec(memory_space=pltpu.SMEM)
    first = state is None
    operands = [device, lengths, first_queries, second_queries, *blocks]
    aliases = {}
    if not first:
        if not last:
            aliases = {len(operands): 0, len(operands) + 1: 1}
        operands += state
    keys = len(blocks) * tokens
    outs = state_shapes
    if last:
        outs = [jax.ShapeDtypeStruct(q.shape, q.dtype) for q in (first_queries, second_queries)]
    return pl.pallas_call(
        functools.partial(attend_kernel, sources, len(blocks), first, last),
        out_shape=outs,
        in_specs=[in_smem, in_smem] + [in_vmem] * (len(operands) - 2),
        out_specs=[in_vmem] * 2,
        scratch_shapes=[pltpu.VMEM((keys, width), jnp.float32)],
        input_output_aliases=aliases,
        cost_estimate=pl.CostEstimate(
            flops=steps * 4 * keys * width * HEAD_WIDTH,
            bytes_accessed=2 * first_queries.size * 2 + 2 * keys * 2 * KEY_VALUE_HEADS * HEAD_WIDTH,
            transcendentals=steps * keys * width,
        ),
        compiler_params=pltpu.CompilerParams(vmem_limit_bytes=16 * 1024 * 1024),
        name="attend_last" if last else "attend",
    )(*operands)


def on_device(first_queries, second_queries, common_keys, common_values, lengths):
    members = lax.axis_size("seq")
    rounds = members // 2 // LEVEL
    device = lax.axis_index("seq").astype(jnp.int32).reshape(1)

    def send(block, route):
        return lax.ppermute(block, "seq", route)

    def core(block):
        return send(block, swapped(members, CORE))

    def row(block):
        return send(block, swapped(members, ROW))

    def behind(levels, flip):
        return lambda d: (d ^ flip) - levels * LEVEL

    def upper_behind(levels, flip):
        return lambda d: jnp.where(d & ROW == 0, (d ^ flip) - levels * LEVEL, NOWHERE)

    own = pack(common_keys, common_values)
    step = functools.partial(attend, device, lengths, first_queries, second_queries)

    previous = send(own, shifted(members))
    beside = row(own)
    partner = core(own)
    state = step([own, partner], [behind(0, 0), behind(0, CORE)], None, False)

    blocks, sources = [beside, core(beside)], [behind(0, ROW), behind(0, ROW | CORE)]
    for level in range(1, rounds):
        blocks += [previous, core(previous)]
        sources += [behind(level, 0), behind(level, CORE)]
        following = send(previous, shifted(members))
        over = row(previous)
        if level == rounds - 1:
            corner = send(previous, across(members))
        state = step(blocks, sources, state, False)
        blocks, sources = [over, core(over)], [behind(level, ROW), behind(level, ROW | CORE)]
        previous = following
    blocks += [previous, core(previous)]
    sources += [behind(rounds, 0), behind(rounds, CORE)]
    state = step(blocks, sources, state, False)
    return tuple(
        step(
            [corner, core(corner)],
            [upper_behind(rounds, ROW), upper_behind(rounds, ROW | CORE)],
            state,
            True,
        )
    )


def solution(mesh):
    tokens = P(("groups", "seq"), None)
    return jax.shard_map(
        on_device,
        mesh=mesh,
        in_specs=(tokens, tokens, tokens, tokens, P("groups")),
        out_specs=(tokens, tokens),
        check_vma=False,
    )
```

```python
import functools
import math

import jax
import jax.numpy as jnp
from jax import lax
from jax.experimental import pallas as pl
from jax.experimental.pallas import tpu as pltpu
from jax.sharding import PartitionSpec as P


HEAD_WIDTH = 128
QUERY_HEAD_COUNT = 16
KEY_VALUE_HEADS = 4

CORE = 1
ROW = 2
LEVEL = 4

HIDDEN = -1e30
NOWHERE = -(1 << 20)
PAIR = 2
AHEAD = 2
BEHIND = 1

GRANT = 16 << 20
SMALL_GRANT = 4 << 20


def swapped(count, distance):
    return [(d, d ^ distance) for d in range(count)]


def shifted(count):
    return [(d, d + LEVEL) for d in range(count - LEVEL)]


def across(count):
    return [(d, d + LEVEL - ROW) for d in range(count - LEVEL) if d & ROW]


def pack_kernel(keys_ref, values_ref, packed_ref, keys_here, values_here, arrived):
    copies = [
        pltpu.make_async_copy(keys_ref, keys_here, arrived.at[0]),
        pltpu.make_async_copy(values_ref, values_here, arrived.at[1]),
    ]
    for copy in copies:
        copy.start()
    copies[0].wait()
    for g in range(KEY_VALUE_HEADS):
        packed_ref[g] = keys_here[:, g * HEAD_WIDTH : (g + 1) * HEAD_WIDTH]
    copies[1].wait()
    for g in range(KEY_VALUE_HEADS):
        packed_ref[KEY_VALUE_HEADS + g] = values_here[:, g * HEAD_WIDTH : (g + 1) * HEAD_WIDTH].T


def pack(keys, values):
    tokens = keys.shape[0]
    return pl.pallas_call(
        pack_kernel,
        out_shape=jax.ShapeDtypeStruct((2 * KEY_VALUE_HEADS, tokens, HEAD_WIDTH), keys.dtype),
        in_specs=[pl.BlockSpec(memory_space=pltpu.HBM)] * 2,
        out_specs=pl.BlockSpec(memory_space=pltpu.VMEM),
        scratch_shapes=[
            pltpu.VMEM(keys.shape, keys.dtype),
            pltpu.VMEM(values.shape, values.dtype),
            pltpu.SemaphoreType.DMA((2,)),
        ],
        compiler_params=pltpu.CompilerParams(vmem_limit_bytes=SMALL_GRANT),
        name="pack",
    )(*[pltpu.with_memory_space_constraint(a, pltpu.HBM) for a in (keys, values)])


def attend_kernel(sources, count, first, last, *refs):
    refs = list(refs)
    device_ref, lengths_ref, first_ref, second_ref = refs[:4]
    blocks = refs[4 : 4 + count]
    rest = refs[4 + count :]
    if not first:
        sum_in, stat_in = rest[:2]
        rest = rest[2:]
    if last:
        gone_refs, rest = rest[:2], rest[2:]
        out_refs, left, rest = rest[:2], rest[2], rest[3:]
    else:
        sum_ref, stat_ref = rest[:2]
        rest = rest[2:]
    (bias_ref,) = rest
    if first:
        sum_in, stat_in = None, None

    tokens = first_ref.shape[0]
    device = device_ref[0]
    query_base = device * tokens
    bounds = []
    total = 0
    for k in range(lengths_ref.shape[0] - 1):
        total = total + lengths_ref[k]
        bounds.append(total)

    def start_of(place):
        start = jnp.zeros_like(place)
        for bound in bounds:
            start = jnp.where(place >= bound, bound, start)
        return start

    bases = [source(device) * tokens for source in sources]
    earliest = start_of(query_base)

    def needed(i):
        return (bases[i] <= query_base + tokens - 1) & (bases[i] + tokens - 1 >= earliest)

    group = QUERY_HEAD_COUNT // KEY_VALUE_HEADS
    pairs = group // PAIR
    steps = [(g, layer, pair) for g in range(KEY_VALUE_HEADS) for layer in range(2) for pair in range(pairs)]
    factor = math.log2(math.e) / math.sqrt(HEAD_WIDTH)

    def scores(step, active):
        g, layer, pair = step
        source = (first_ref, second_ref)[layer]
        head = g * group + pair * PAIR
        query = jnp.concatenate(
            [source[:, (head + i) * HEAD_WIDTH : (head + i + 1) * HEAD_WIDTH] for i in range(PAIR)], axis=0
        )
        keys = jnp.concatenate([blocks[i][g] for i in active], axis=0)
        return lax.dot_general(keys, query, (((1,), (1,)), ((), ())), preferred_element_type=jnp.float32)

    def weigh(n, raw):
        masked = raw * factor + bias_ref[: raw.shape[0], :]
        highest = jnp.max(masked, axis=0, keepdims=True)
        fade = None
        if not first:
            former = stat_in[2 * n : 2 * n + 1, :]
            highest = jnp.maximum(highest, former)
            fade = jnp.exp2(former - highest)
        weights = jnp.exp2(masked - highest)
        row_sum = jnp.sum(weights, axis=0, keepdims=True)
        return n, weights.astype(jnp.bfloat16), highest, fade, row_sum

    def gather(active, n, rounded, highest, fade, row_sum):
        values = jnp.concatenate([blocks[i][KEY_VALUE_HEADS + steps[n][0]] for i in active], axis=1)
        product = jnp.dot(values, rounded, preferred_element_type=jnp.float32)
        if not first:
            row_sum = row_sum + stat_in[2 * n + 1 : 2 * n + 2, :] * fade
            product = product + sum_in[n] * fade
        finish(n, steps[n], product, row_sum, highest)

    def absorb(active):
        place = query_base + lax.broadcasted_iota(jnp.int32, (1, tokens), 1)
        start = start_of(place)
        for row, i in enumerate(active):
            key_place = bases[i] + lax.broadcasted_iota(jnp.int32, (tokens, tokens), 0)
            visible = (key_place >= start) & (key_place <= place)
            bias = jnp.where(visible, 0.0, HIDDEN)
            for j in range(PAIR):
                bias_ref[row * tokens : (row + 1) * tokens, j * tokens : (j + 1) * tokens] = bias

        early = [scores(step, active) for step in steps[:AHEAD]]
        late = []
        for n in range(len(steps)):
            if n + AHEAD < len(steps):
                early.append(scores(steps[n + AHEAD], active))
            if len(late) > BEHIND:
                gather(active, *late.pop(0))
            late.append(weigh(n, early.pop(0)))
        for item in late:
            gather(active, *item)

    def leaving(n):
        g, layer, pair = steps[n]
        columns = pl.ds((g * group + pair * PAIR) * HEAD_WIDTH, PAIR * HEAD_WIDTH)
        return pltpu.make_async_copy(out_refs[layer].at[:, columns], gone_refs[layer].at[:, columns], left.at[n])

    def finish(n, step, product, row_sum, highest):
        g, layer, pair = step
        if last:
            blended = (product * (1.0 / row_sum)).astype(jnp.bfloat16)
            head = g * group + pair * PAIR
            for i in range(PAIR):
                columns = slice((head + i) * HEAD_WIDTH, (head + i + 1) * HEAD_WIDTH)
                out_refs[layer][:, columns] = blended[:, i * tokens : (i + 1) * tokens].T
            leaving(n).start()
        else:
            sum_ref[n] = product
            stat_ref[2 * n : 2 * n + 1, :] = highest
            stat_ref[2 * n + 1 : 2 * n + 2, :] = row_sum

    if first:
        both = needed(1)
        pl.when(both)(lambda: absorb([0, 1]))
        pl.when(jnp.logical_not(both))(lambda: absorb([0]))
        return

    near = needed(0) | needed(1)
    far = needed(count - 2) | needed(count - 1)
    if count > 2:
        pl.when(near & far)(lambda: absorb(list(range(count))))
        pl.when(near & jnp.logical_not(far))(lambda: absorb([0, 1]))
        pl.when(far & jnp.logical_not(near))(lambda: absorb([count - 2, count - 1]))
    else:
        pl.when(near)(lambda: absorb([0, 1]))

    @pl.when(jnp.logical_not(near | far))
    def _():
        for n, step in enumerate(steps):
            finish(n, step, sum_in[n], stat_in[2 * n + 1 : 2 * n + 2, :], stat_in[2 * n : 2 * n + 1, :])

    if last:
        for n in range(len(steps)):
            leaving(n).wait()


def attend(device, lengths, first_queries, second_queries, blocks, sources, state, last):
    tokens = first_queries.shape[0]
    steps = 2 * QUERY_HEAD_COUNT // PAIR
    width = PAIR * tokens
    state_shapes = [
        jax.ShapeDtypeStruct((steps, HEAD_WIDTH, width), jnp.float32),
        jax.ShapeDtypeStruct((2 * steps, width), jnp.float32),
    ]
    in_vmem = pl.BlockSpec(memory_space=pltpu.VMEM)
    in_smem = pl.BlockSpec(memory_space=pltpu.SMEM)
    first = state is None
    operands = [device, lengths, first_queries, second_queries, *blocks]
    aliases = {}
    if not first:
        if not last:
            aliases = {len(operands): 0, len(operands) + 1: 1}
        operands += state
    keys = len(blocks) * tokens
    outs = state_shapes
    if last:
        outs = [jax.ShapeDtypeStruct(q.shape, q.dtype) for q in (first_queries, second_queries)]
    leaving = [pltpu.VMEM(q.shape, q.dtype) for q in (first_queries, second_queries)]
    leaving.append(pltpu.SemaphoreType.DMA((steps,)))
    return pl.pallas_call(
        functools.partial(attend_kernel, sources, len(blocks), first, last),
        out_shape=outs,
        in_specs=[in_smem, in_smem] + [in_vmem] * (len(operands) - 2),
        out_specs=[pl.BlockSpec(memory_space=pltpu.HBM) if last else in_vmem] * 2,
        scratch_shapes=[
            *(leaving if last else []),
            pltpu.VMEM((keys, width), jnp.float32),
        ],
        input_output_aliases=aliases,
        cost_estimate=pl.CostEstimate(
            flops=steps * 4 * keys * width * HEAD_WIDTH,
            bytes_accessed=2 * first_queries.size * 2 + 2 * keys * 2 * KEY_VALUE_HEADS * HEAD_WIDTH,
            transcendentals=steps * keys * width,
        ),
        compiler_params=pltpu.CompilerParams(vmem_limit_bytes=GRANT),
        name="attend_last" if last else "attend",
    )(*operands)


def on_device(first_queries, second_queries, common_keys, common_values, lengths):
    members = lax.axis_size("seq")
    rounds = members // 2 // LEVEL
    device = lax.axis_index("seq").astype(jnp.int32).reshape(1)

    def send(block, route):
        return lax.ppermute(block, "seq", route)

    def core(block):
        return send(block, swapped(members, CORE))

    def row(block):
        return send(block, swapped(members, ROW))

    def behind(levels, flip):
        return lambda d: (d ^ flip) - levels * LEVEL

    def upper_behind(levels, flip):
        return lambda d: jnp.where(d & ROW == 0, (d ^ flip) - levels * LEVEL, NOWHERE)

    own = pack(common_keys, common_values)
    step = functools.partial(attend, device, lengths, first_queries, second_queries)

    previous = send(own, shifted(members))
    beside = row(own)
    partner = core(own)
    state = step([own, partner], [behind(0, 0), behind(0, CORE)], None, False)

    blocks, sources = [beside, core(beside)], [behind(0, ROW), behind(0, ROW | CORE)]
    for level in range(1, rounds):
        blocks += [previous, core(previous)]
        sources += [behind(level, 0), behind(level, CORE)]
        following = send(previous, shifted(members))
        over = row(previous)
        if level == rounds - 1:
            corner = send(previous, across(members))
        state = step(blocks, sources, state, False)
        blocks, sources = [over, core(over)], [behind(level, ROW), behind(level, ROW | CORE)]
        previous = following
    blocks += [previous, core(previous)]
    sources += [behind(rounds, 0), behind(rounds, CORE)]
    state = step(blocks, sources, state, False)
    return tuple(
        step(
            [corner, core(corner)],
            [upper_behind(rounds, ROW), upper_behind(rounds, ROW | CORE)],
            state,
            True,
        )
    )


def solution(mesh):
    tokens = P(("groups", "seq"), None)
    return jax.shard_map(
        on_device,
        mesh=mesh,
        in_specs=(tokens, tokens, tokens, tokens, P("groups")),
        out_specs=(tokens, tokens),
        check_vma=False,
    )
```

```python
import functools
import math

import jax
import jax.numpy as jnp
from jax import lax
from jax.experimental import pallas as pl
from jax.experimental.pallas import tpu as pltpu
from jax.sharding import PartitionSpec as P


HEAD_WIDTH = 128
QUERY_HEAD_COUNT = 16
KEY_VALUE_HEADS = 4

CORE = 1
ROW = 2
LEVEL = 4

HIDDEN = -1e30
NOWHERE = -(1 << 20)
PAIR = 2
BEHIND = 1

ONES = 16

GRANT = 16 << 20
SMALL_GRANT = 4 << 20


def swapped(count, distance):
    return [(d, d ^ distance) for d in range(count)]


def shifted(count):
    return [(d, (d + LEVEL) % count) for d in range(count)]


def across(count, held):
    last = count - LEVEL
    route = [(d, d ^ ROW) for d in range(held * LEVEL)]
    for d in range(held * LEVEL, count):
        if not d & ROW:
            route.append((d, d + ROW))
        elif d < last:
            route.append((d, d + LEVEL - ROW))
        else:
            route.append((d, held * LEVEL + d - last - ROW))
    return route


def pack_kernel(keys_ref, values_ref, packed_ref, keys_here, values_here, arrived):
    copies = [
        pltpu.make_async_copy(keys_ref, keys_here, arrived.at[0]),
        pltpu.make_async_copy(values_ref, values_here, arrived.at[1]),
    ]
    for copy in copies:
        copy.start()
    copies[0].wait()
    for g in range(KEY_VALUE_HEADS):
        packed_ref[g] = keys_here[:, g * HEAD_WIDTH : (g + 1) * HEAD_WIDTH]
    copies[1].wait()
    for g in range(KEY_VALUE_HEADS):
        packed_ref[KEY_VALUE_HEADS + g] = values_here[:, g * HEAD_WIDTH : (g + 1) * HEAD_WIDTH].T


def pack(keys, values):
    tokens = keys.shape[0]
    return pl.pallas_call(
        pack_kernel,
        out_shape=jax.ShapeDtypeStruct((2 * KEY_VALUE_HEADS, tokens, HEAD_WIDTH), keys.dtype),
        in_specs=[pl.BlockSpec(memory_space=pltpu.HBM)] * 2,
        out_specs=pl.BlockSpec(memory_space=pltpu.VMEM),
        scratch_shapes=[
            pltpu.VMEM(keys.shape, keys.dtype),
            pltpu.VMEM(values.shape, values.dtype),
            pltpu.SemaphoreType.DMA((2,)),
        ],
        compiler_params=pltpu.CompilerParams(vmem_limit_bytes=SMALL_GRANT),
        name="pack",
    )(*[pltpu.with_memory_space_constraint(a, pltpu.HBM) for a in (keys, values)])


def attend_kernel(sources, count, first, last, *refs):
    refs = list(refs)
    device_ref, lengths_ref, first_ref, second_ref = refs[:4]
    blocks = refs[4 : 4 + count]
    rest = refs[4 + count :]
    if not first:
        sum_in, stat_in = rest[:2]
        rest = rest[2:]
    if last:
        gone_refs, rest = rest[:2], rest[2:]
        out_refs, left, rest = rest[:2], rest[2], rest[3:]
    else:
        sum_ref, stat_ref = rest[:2]
        rest = rest[2:]
    (bias_ref,) = rest
    if first:
        sum_in, stat_in = None, None

    tokens = first_ref.shape[0]
    device = device_ref[0]
    query_base = device * tokens
    bounds = []
    total = 0
    for k in range(lengths_ref.shape[0] - 1):
        total = total + lengths_ref[k]
        bounds.append(total)

    def start_of(place):
        start = jnp.zeros_like(place)
        for bound in bounds:
            start = jnp.where(place >= bound, bound, start)
        return start

    bases = [source(device) * tokens for source in sources]
    earliest = start_of(query_base)

    def needed(i):
        return (bases[i] <= query_base + tokens - 1) & (bases[i] + tokens - 1 >= earliest)

    group = QUERY_HEAD_COUNT // KEY_VALUE_HEADS
    pairs = group // PAIR
    steps = [(g, layer, pair) for g in range(KEY_VALUE_HEADS) for layer in range(2) for pair in range(pairs)]
    factor = math.log2(math.e) / math.sqrt(HEAD_WIDTH)

    def scores(step, active):
        g, layer, pair = step
        source = (first_ref, second_ref)[layer]
        head = g * group + pair * PAIR
        query = jnp.concatenate(
            [source[:, (head + i) * HEAD_WIDTH : (head + i + 1) * HEAD_WIDTH] for i in range(PAIR)], axis=0
        )
        keys = jnp.concatenate([blocks[i][g] for i in active], axis=0)
        return lax.dot_general(keys, query, (((1,), (1,)), ((), ())), preferred_element_type=jnp.float32)

    def weigh(n, raw):
        masked = raw * factor + bias_ref[: raw.shape[0], :]
        highest = jnp.max(masked, axis=0, keepdims=True)
        fade = None
        if not first:
            former = stat_in[2 * n : 2 * n + 1, :]
            highest = jnp.maximum(highest, former)
            fade = jnp.exp2(former - highest)
        weights = jnp.exp2(masked - highest)
        return n, weights.astype(jnp.bfloat16), highest, fade

    def gather(active, n, rounded, highest, fade):
        values = jnp.concatenate([blocks[i][KEY_VALUE_HEADS + steps[n][0]] for i in active], axis=1)
        values = jnp.concatenate([values, jnp.ones((ONES, values.shape[1]), values.dtype)], axis=0)
        product = jnp.dot(values, rounded, preferred_element_type=jnp.float32)
        product, row_sum = product[:HEAD_WIDTH], product[HEAD_WIDTH : HEAD_WIDTH + 1]
        if not first:
            row_sum = row_sum + stat_in[2 * n + 1 : 2 * n + 2, :] * fade
            product = product + sum_in[n] * fade
        finish(n, steps[n], product, row_sum, highest)

    def absorb(active):
        place = query_base + lax.broadcasted_iota(jnp.int32, (1, tokens), 1)
        start = start_of(place)
        for row, i in enumerate(active):
            key_place = bases[i] + lax.broadcasted_iota(jnp.int32, (tokens, tokens), 0)
            visible = (key_place >= start) & (key_place <= place)
            bias = jnp.where(visible, 0.0, HIDDEN)
            for j in range(PAIR):
                bias_ref[row * tokens : (row + 1) * tokens, j * tokens : (j + 1) * tokens] = bias

        ahead = 1 if len(active) > 2 else 3
        early = [scores(step, active) for step in steps[:ahead]]
        late = []
        for n in range(len(steps)):
            if n + ahead < len(steps):
                early.append(scores(steps[n + ahead], active))
            if len(late) > BEHIND:
                gather(active, *late.pop(0))
            late.append(weigh(n, early.pop(0)))
        for item in late:
            gather(active, *item)

    def leaving(n):
        g, layer, pair = steps[n]
        columns = pl.ds((g * group + pair * PAIR) * HEAD_WIDTH, PAIR * HEAD_WIDTH)
        return pltpu.make_async_copy(out_refs[layer].at[:, columns], gone_refs[layer].at[:, columns], left.at[n])

    def finish(n, step, product, row_sum, highest):
        g, layer, pair = step
        if last:
            blended = (product * (1.0 / row_sum)).astype(jnp.bfloat16)
            head = g * group + pair * PAIR
            for i in range(PAIR):
                columns = slice((head + i) * HEAD_WIDTH, (head + i + 1) * HEAD_WIDTH)
                out_refs[layer][:, columns] = blended[:, i * tokens : (i + 1) * tokens].T
            leaving(n).start()
        else:
            sum_ref[n] = product
            stat_ref[2 * n : 2 * n + 1, :] = highest
            stat_ref[2 * n + 1 : 2 * n + 2, :] = row_sum

    if first:
        both = needed(1)
        pl.when(both)(lambda: absorb([0, 1]))
        pl.when(jnp.logical_not(both))(lambda: absorb([0]))
        return

    near = needed(0) | needed(1)
    far = needed(count - 2) | needed(count - 1)
    if count > 2:
        pl.when(near & far)(lambda: absorb(list(range(count))))
        pl.when(near & jnp.logical_not(far))(lambda: absorb([0, 1]))
        pl.when(far & jnp.logical_not(near))(lambda: absorb([count - 2, count - 1]))
    else:
        pl.when(near)(lambda: absorb([0, 1]))

    @pl.when(jnp.logical_not(near | far))
    def _():
        for n, step in enumerate(steps):
            finish(n, step, sum_in[n], stat_in[2 * n + 1 : 2 * n + 2, :], stat_in[2 * n : 2 * n + 1, :])

    if last:
        for n in range(len(steps)):
            leaving(n).wait()


def attend(device, lengths, first_queries, second_queries, blocks, sources, state, last):
    tokens = first_queries.shape[0]
    steps = 2 * QUERY_HEAD_COUNT // PAIR
    width = PAIR * tokens
    state_shapes = [
        jax.ShapeDtypeStruct((steps, HEAD_WIDTH, width), jnp.float32),
        jax.ShapeDtypeStruct((2 * steps, width), jnp.float32),
    ]
    in_vmem = pl.BlockSpec(memory_space=pltpu.VMEM)
    in_smem = pl.BlockSpec(memory_space=pltpu.SMEM)
    first = state is None
    operands = [device, lengths, first_queries, second_queries, *blocks]
    aliases = {}
    if not first:
        if not last:
            aliases = {len(operands): 0, len(operands) + 1: 1}
        operands += state
    keys = len(blocks) * tokens
    outs = state_shapes
    if last:
        outs = [jax.ShapeDtypeStruct(q.shape, q.dtype) for q in (first_queries, second_queries)]
    leaving = [pltpu.VMEM(q.shape, q.dtype) for q in (first_queries, second_queries)]
    leaving.append(pltpu.SemaphoreType.DMA((steps,)))
    return pl.pallas_call(
        functools.partial(attend_kernel, sources, len(blocks), first, last),
        out_shape=outs,
        in_specs=[in_smem, in_smem] + [in_vmem] * (len(operands) - 2),
        out_specs=[pl.BlockSpec(memory_space=pltpu.HBM) if last else in_vmem] * 2,
        scratch_shapes=[
            *(leaving if last else []),
            pltpu.VMEM((keys, width), jnp.float32),
        ],
        input_output_aliases=aliases,
        cost_estimate=pl.CostEstimate(
            flops=steps * 4 * keys * width * HEAD_WIDTH,
            bytes_accessed=2 * first_queries.size * 2 + 2 * keys * 2 * KEY_VALUE_HEADS * HEAD_WIDTH,
            transcendentals=steps * keys * width,
        ),
        compiler_params=pltpu.CompilerParams(vmem_limit_bytes=GRANT),
        name="attend_last" if last else "attend",
    )(*operands)


def on_device(first_queries, second_queries, common_keys, common_values, lengths):
    members = lax.axis_size("seq")
    rounds = members // 2 // LEVEL
    device = lax.axis_index("seq").astype(jnp.int32).reshape(1)

    def send(block, route):
        return lax.ppermute(block, "seq", route)

    def core(block):
        return send(block, swapped(members, CORE))

    def row(block):
        return send(block, swapped(members, ROW))

    def behind(levels, flip):
        return lambda d: (d ^ flip) - levels * LEVEL

    def upper_behind(levels, flip):
        return lambda d: jnp.where(d & ROW == 0, (d ^ flip) - levels * LEVEL, NOWHERE)

    own = pack(common_keys, common_values)
    step = functools.partial(attend, device, lengths, first_queries, second_queries)
    previous = send(own, shifted(members))
    beside = row(own)
    partner = core(own)
    state = step([own, partner], [behind(0, 0), behind(0, CORE)], None, False)

    blocks, sources = [beside, core(beside)], [behind(0, ROW), behind(0, ROW | CORE)]
    for level in range(1, rounds):
        blocks += [previous, core(previous)]
        sources += [behind(level, 0), behind(level, CORE)]
        following = send(previous, shifted(members))
        over = row(previous)
        if level == rounds - 1:
            corner = send(previous, across(members, level))
        state = step(blocks, sources, state, False)
        blocks, sources = [over, core(over)], [behind(level, ROW), behind(level, ROW | CORE)]
        previous = following
    blocks += [previous, core(previous)]
    sources += [behind(rounds, 0), behind(rounds, CORE)]
    state = step(blocks, sources, state, False)
    return tuple(
        step(
            [corner, core(corner)],
            [upper_behind(rounds, ROW), upper_behind(rounds, ROW | CORE)],
            state,
            True,
        )
    )


def solution(mesh):
    tokens = P(("groups", "seq"), None)
    return jax.shard_map(
        on_device,
        mesh=mesh,
        in_specs=(tokens, tokens, tokens, tokens, P("groups")),
        out_specs=(tokens, tokens),
        check_vma=False,
    )
```

```python
import functools
import math

import jax
import jax.numpy as jnp
from jax import lax
from jax.experimental import pallas as pl
from jax.experimental.pallas import tpu as pltpu
from jax.sharding import PartitionSpec as P


HEAD_WIDTH = 128
QUERY_HEAD_COUNT = 16
KEY_VALUE_HEADS = 4

CORE = 1
ROW = 2
LEVEL = 4

HIDDEN = -1e30
NOWHERE = -(1 << 20)
PAIR = 2
BEHIND = 1

ONES = 16

GRANT = 16 << 20
SMALL_GRANT = 4 << 20


def swapped(count, distance):
    return [(d, d ^ distance) for d in range(count)]


def shifted(count):
    return [(d, (d + LEVEL) % count) for d in range(count)]


def across(count, held):
    last = count - LEVEL
    route = [(d, d ^ ROW) for d in range(held * LEVEL)]
    for d in range(held * LEVEL, count):
        if not d & ROW:
            route.append((d, d + ROW))
        elif d < last:
            route.append((d, d + LEVEL - ROW))
        else:
            route.append((d, held * LEVEL + d - last - ROW))
    return route


def pack_kernel(keys_ref, values_ref, packed_ref, keys_here, values_here, arrived):
    copies = [
        pltpu.make_async_copy(keys_ref, keys_here, arrived.at[0]),
        pltpu.make_async_copy(values_ref, values_here, arrived.at[1]),
    ]
    for copy in copies:
        copy.start()
    copies[0].wait()
    for g in range(KEY_VALUE_HEADS):
        packed_ref[g] = keys_here[:, g * HEAD_WIDTH : (g + 1) * HEAD_WIDTH]
    copies[1].wait()
    for g in range(KEY_VALUE_HEADS):
        packed_ref[KEY_VALUE_HEADS + g] = values_here[:, g * HEAD_WIDTH : (g + 1) * HEAD_WIDTH].T


def pack(keys, values):
    tokens = keys.shape[0]
    return pl.pallas_call(
        pack_kernel,
        out_shape=jax.ShapeDtypeStruct((2 * KEY_VALUE_HEADS, tokens, HEAD_WIDTH), keys.dtype),
        in_specs=[pl.BlockSpec(memory_space=pltpu.HBM)] * 2,
        out_specs=pl.BlockSpec(memory_space=pltpu.VMEM),
        scratch_shapes=[
            pltpu.VMEM(keys.shape, keys.dtype),
            pltpu.VMEM(values.shape, values.dtype),
            pltpu.SemaphoreType.DMA((2,)),
        ],
        compiler_params=pltpu.CompilerParams(vmem_limit_bytes=SMALL_GRANT),
        name="pack",
    )(*[pltpu.with_memory_space_constraint(a, pltpu.HBM) for a in (keys, values)])


def attend_kernel(sources, later, count, first, last, *refs):
    refs = list(refs)
    device_ref, lengths_ref, first_ref, second_ref = refs[:4]
    blocks = refs[4 : 4 + count]
    rest = refs[4 + count :]
    if not first:
        sum_in, stat_in = rest[:2]
        rest = rest[2:]
    if last:
        rest = rest[2:]
    else:
        sum_ref, stat_ref = rest[:2]
        rest = rest[2:]
    if last or later:
        gone_refs, out_refs, left, rest = rest[:2], rest[2:4], rest[4], rest[5:]
    (bias_ref,) = rest
    if first:
        sum_in, stat_in = None, None

    tokens = first_ref.shape[0]
    device = device_ref[0]
    query_base = device * tokens
    bounds = []
    total = 0
    for k in range(lengths_ref.shape[0] - 1):
        total = total + lengths_ref[k]
        bounds.append(total)

    def start_of(place):
        start = jnp.zeros_like(place)
        for bound in bounds:
            start = jnp.where(place >= bound, bound, start)
        return start

    bases = [source(device) * tokens for source in sources]
    earliest = start_of(query_base)

    def seen(base):
        return (base <= query_base + tokens - 1) & (base + tokens - 1 >= earliest)

    def needed(i):
        return seen(bases[i])

    group = QUERY_HEAD_COUNT // KEY_VALUE_HEADS
    pairs = group // PAIR
    steps = [(g, layer, pair) for g in range(KEY_VALUE_HEADS) for layer in range(2) for pair in range(pairs)]
    factor = math.log2(math.e) / math.sqrt(HEAD_WIDTH)

    def scores(step, active):
        g, layer, pair = step
        source = (first_ref, second_ref)[layer]
        head = g * group + pair * PAIR
        query = jnp.concatenate(
            [source[:, (head + i) * HEAD_WIDTH : (head + i + 1) * HEAD_WIDTH] for i in range(PAIR)], axis=0
        )
        keys = jnp.concatenate([blocks[i][g] for i in active], axis=0)
        return lax.dot_general(keys, query, (((1,), (1,)), ((), ())), preferred_element_type=jnp.float32)

    def weigh(n, raw):
        masked = raw * factor + bias_ref[: raw.shape[0], :]
        highest = jnp.max(masked, axis=0, keepdims=True)
        fade = None
        if not first:
            former = stat_in[2 * n : 2 * n + 1, :]
            highest = jnp.maximum(highest, former)
            fade = jnp.exp2(former - highest)
        weights = jnp.exp2(masked - highest)
        return n, weights.astype(jnp.bfloat16), highest, fade

    def gather(active, n, rounded, highest, fade):
        values = jnp.concatenate([blocks[i][KEY_VALUE_HEADS + steps[n][0]] for i in active], axis=1)
        values = jnp.concatenate([values, jnp.ones((ONES, values.shape[1]), values.dtype)], axis=0)
        product = jnp.dot(values, rounded, preferred_element_type=jnp.float32)
        product, row_sum = product[:HEAD_WIDTH], product[HEAD_WIDTH : HEAD_WIDTH + 1]
        if not first:
            row_sum = row_sum + stat_in[2 * n + 1 : 2 * n + 2, :] * fade
            product = product + sum_in[n] * fade
        finish(n, steps[n], product, row_sum, highest)

    def absorb(active):
        place = query_base + lax.broadcasted_iota(jnp.int32, (1, tokens), 1)
        start = start_of(place)
        for row, i in enumerate(active):
            key_place = bases[i] + lax.broadcasted_iota(jnp.int32, (tokens, tokens), 0)
            visible = (key_place >= start) & (key_place <= place)
            bias = jnp.where(visible, 0.0, HIDDEN)
            for j in range(PAIR):
                bias_ref[row * tokens : (row + 1) * tokens, j * tokens : (j + 1) * tokens] = bias

        ahead = 1 if len(active) > 2 else 3
        early = [scores(step, active) for step in steps[:ahead]]
        late = []
        for n in range(len(steps)):
            if n + ahead < len(steps):
                early.append(scores(steps[n + ahead], active))
            if len(late) > BEHIND:
                gather(active, *late.pop(0))
            late.append(weigh(n, early.pop(0)))
        for item in late:
            gather(active, *item)

    def leaving(n):
        g, layer, pair = steps[n]
        columns = pl.ds((g * group + pair * PAIR) * HEAD_WIDTH, PAIR * HEAD_WIDTH)
        return pltpu.make_async_copy(out_refs[layer].at[:, columns], gone_refs[layer].at[:, columns], left.at[n])

    def settle(n, step, product, row_sum):
            g, layer, pair = step
            blended = (product * (1.0 / row_sum)).astype(jnp.bfloat16)
            head = g * group + pair * PAIR
            for i in range(PAIR):
                columns = slice((head + i) * HEAD_WIDTH, (head + i + 1) * HEAD_WIDTH)
                out_refs[layer][:, columns] = blended[:, i * tokens : (i + 1) * tokens].T
            leaving(n).start()

    def depart():
        for n in range(len(steps)):
            leaving(n).wait()

    def finish(n, step, product, row_sum, highest):
        if last:
            settle(n, step, product, row_sum)
        else:
            sum_ref[n] = product
            stat_ref[2 * n : 2 * n + 1, :] = highest
            stat_ref[2 * n + 1 : 2 * n + 2, :] = row_sum

    if first:
        both = needed(1)
        pl.when(both)(lambda: absorb([0, 1]))
        pl.when(jnp.logical_not(both))(lambda: absorb([0]))
        return

    near = needed(0) | needed(1)
    if last:

        @pl.when(near)
        def _():
            absorb([0, 1])
            depart()

        return

    far = needed(count - 2) | needed(count - 1)
    pl.when(near & far)(lambda: absorb(list(range(count))))
    pl.when(near & jnp.logical_not(far))(lambda: absorb([0, 1]))
    pl.when(far & jnp.logical_not(near))(lambda: absorb([count - 2, count - 1]))

    @pl.when(jnp.logical_not(near | far))
    def _():
        for n, step in enumerate(steps):
            finish(n, step, sum_in[n], stat_in[2 * n + 1 : 2 * n + 2, :], stat_in[2 * n : 2 * n + 1, :])

    if later:
        awaited = functools.reduce(jnp.logical_or, [seen(source(device) * tokens) for source in later])

        @pl.when(jnp.logical_not(awaited))
        def _():
            for n, step in enumerate(steps):
                settle(n, step, sum_ref[n], stat_ref[2 * n + 1 : 2 * n + 2, :])
            depart()


def attend(device, lengths, first_queries, second_queries, blocks, sources, state, later=(), outputs=()):
    tokens = first_queries.shape[0]
    steps = 2 * QUERY_HEAD_COUNT // PAIR
    width = PAIR * tokens
    state_shapes = [
        jax.ShapeDtypeStruct((steps, HEAD_WIDTH, width), jnp.float32),
        jax.ShapeDtypeStruct((2 * steps, width), jnp.float32),
    ]
    in_vmem = pl.BlockSpec(memory_space=pltpu.VMEM)
    in_smem = pl.BlockSpec(memory_space=pltpu.SMEM)
    first = state is None
    last = bool(outputs)
    in_hbm = pl.BlockSpec(memory_space=pltpu.HBM)
    operands = [device, lengths, first_queries, second_queries, *blocks]
    aliases = {}
    if not first:
        if not last:
            aliases = {len(operands): 0, len(operands) + 1: 1}
        operands += state
    if last:
        aliases = {len(operands): 0, len(operands) + 1: 1}
        operands += outputs
    keys = len(blocks) * tokens
    outs = [jax.ShapeDtypeStruct(q.shape, q.dtype) for q in (first_queries, second_queries)]
    if not last:
        outs = state_shapes + (outs if later else [])
    leaving = [pltpu.VMEM(q.shape, q.dtype) for q in (first_queries, second_queries)]
    leaving.append(pltpu.SemaphoreType.DMA((steps,)))
    return pl.pallas_call(
        functools.partial(attend_kernel, sources, later, len(blocks), first, last),
        out_shape=outs,
        in_specs=[in_smem, in_smem] + [in_vmem] * (len(operands) - 2 - len(outputs)) + [in_hbm] * len(outputs),
        out_specs=[in_hbm] * 2 if last else [in_vmem] * 2 + [in_hbm] * (len(outs) - 2),
        scratch_shapes=[
            *(leaving if last or later else []),
            pltpu.VMEM((keys, width), jnp.float32),
        ],
        input_output_aliases=aliases,
        cost_estimate=pl.CostEstimate(
            flops=steps * 4 * keys * width * HEAD_WIDTH,
            bytes_accessed=2 * first_queries.size * 2 + 2 * keys * 2 * KEY_VALUE_HEADS * HEAD_WIDTH,
            transcendentals=steps * keys * width,
        ),
        compiler_params=pltpu.CompilerParams(vmem_limit_bytes=GRANT),
        name="attend_last" if last else "attend",
    )(*operands)


def on_device(first_queries, second_queries, common_keys, common_values, lengths):
    members = lax.axis_size("seq")
    rounds = members // 2 // LEVEL
    device = lax.axis_index("seq").astype(jnp.int32).reshape(1)

    def send(block, route):
        return lax.ppermute(block, "seq", route)

    def core(block):
        return send(block, swapped(members, CORE))

    def row(block):
        return send(block, swapped(members, ROW))

    def behind(levels, flip):
        return lambda d: (d ^ flip) - levels * LEVEL

    def upper_behind(levels, flip):
        return lambda d: jnp.where(d & ROW == 0, (d ^ flip) - levels * LEVEL, NOWHERE)

    own = pack(common_keys, common_values)
    step = functools.partial(attend, device, lengths, first_queries, second_queries)
    previous = send(own, shifted(members))
    beside = row(own)
    partner = core(own)
    state = step([own, partner], [behind(0, 0), behind(0, CORE)], None)

    blocks, sources = [beside, core(beside)], [behind(0, ROW), behind(0, ROW | CORE)]
    for level in range(1, rounds):
        blocks += [previous, core(previous)]
        sources += [behind(level, 0), behind(level, CORE)]
        following = send(previous, shifted(members))
        over = row(previous)
        if level == rounds - 1:
            corner = send(previous, across(members, level))
        state = step(blocks, sources, state)
        blocks, sources = [over, core(over)], [behind(level, ROW), behind(level, ROW | CORE)]
        previous = following
    blocks += [previous, core(previous)]
    sources += [behind(rounds, 0), behind(rounds, CORE)]
    later = [upper_behind(rounds, ROW), upper_behind(rounds, ROW | CORE)]
    *state, first_output, second_output = step(blocks, sources, state, later)
    blocks = [corner, core(corner)]
    return tuple(step(blocks, later, state, outputs=[first_output, second_output]))


def solution(mesh):
    tokens = P(("groups", "seq"), None)
    return jax.shard_map(
        on_device,
        mesh=mesh,
        in_specs=(tokens, tokens, tokens, tokens, P("groups")),
        out_specs=(tokens, tokens),
        check_vma=False,
    )
```

```python
import functools
import math

import jax
import jax.numpy as jnp
from jax import lax
from jax.experimental import pallas as pl
from jax.experimental.pallas import tpu as pltpu
from jax.sharding import PartitionSpec as P


HEAD_WIDTH = 128
QUERY_HEAD_COUNT = 16
KEY_VALUE_HEADS = 4

CORE = 1
ROW = 2
LEVEL = 4

HIDDEN = -1e30
NOWHERE = -(1 << 20)
PAIR = 2
BEHIND = 1

ONES = 16

GRANT = 16 << 20
SMALL_GRANT = 4 << 20


def swapped(count, distance):
    return [(d, d ^ distance) for d in range(count)]


def shifted(count):
    return [(d, (d + LEVEL) % count) for d in range(count)]


def across(count, held):
    last = count - LEVEL
    route = [(d, d ^ ROW) for d in range(held * LEVEL)]
    for d in range(held * LEVEL, count):
        if not d & ROW:
            route.append((d, d + ROW))
        elif d < last:
            route.append((d, d + LEVEL - ROW))
        else:
            route.append((d, held * LEVEL + d - last - ROW))
    return route


def pack_kernel(keys_ref, values_ref, packed_ref, keys_here, values_here, arrived):
    copies = [
        pltpu.make_async_copy(keys_ref, keys_here, arrived.at[0]),
        pltpu.make_async_copy(values_ref, values_here, arrived.at[1]),
    ]
    for copy in copies:
        copy.start()
    copies[0].wait()
    for g in range(KEY_VALUE_HEADS):
        packed_ref[g] = keys_here[:, g * HEAD_WIDTH : (g + 1) * HEAD_WIDTH]
    copies[1].wait()
    for g in range(KEY_VALUE_HEADS):
        packed_ref[KEY_VALUE_HEADS + g] = values_here[:, g * HEAD_WIDTH : (g + 1) * HEAD_WIDTH].T


def pack(keys, values):
    tokens = keys.shape[0]
    return pl.pallas_call(
        pack_kernel,
        out_shape=jax.ShapeDtypeStruct((2 * KEY_VALUE_HEADS, tokens, HEAD_WIDTH), keys.dtype),
        in_specs=[pl.BlockSpec(memory_space=pltpu.HBM)] * 2,
        out_specs=pl.BlockSpec(memory_space=pltpu.VMEM),
        scratch_shapes=[
            pltpu.VMEM(keys.shape, keys.dtype),
            pltpu.VMEM(values.shape, values.dtype),
            pltpu.SemaphoreType.DMA((2,)),
        ],
        compiler_params=pltpu.CompilerParams(vmem_limit_bytes=SMALL_GRANT),
        name="pack",
    )(*[pltpu.with_memory_space_constraint(a, pltpu.HBM) for a in (keys, values)])


def attend_kernel(sources, later, count, first, last, *refs):
    refs = list(refs)
    device_ref, lengths_ref, first_ref, second_ref = refs[:4]
    blocks = refs[4 : 4 + count]
    rest = refs[4 + count :]
    if not first:
        sum_in, stat_in = rest[:2]
        rest = rest[2:]
    if last:
        rest = rest[2:]
    else:
        sum_ref, stat_ref = rest[:2]
        rest = rest[2:]
    if last or later:
        gone_refs, out_refs, left, rest = rest[:2], rest[2:4], rest[4], rest[5:]
    (bias_ref,) = rest
    if first:
        sum_in, stat_in = None, None

    tokens = first_ref.shape[0]
    device = device_ref[0]
    query_base = device * tokens
    bounds = []
    total = 0
    for k in range(lengths_ref.shape[0] - 1):
        total = total + lengths_ref[k]
        bounds.append(total)

    def start_of(place):
        start = jnp.zeros_like(place)
        for bound in bounds:
            start = jnp.where(place >= bound, bound, start)
        return start

    bases = [source(device) * tokens for source in sources]
    earliest = start_of(query_base)

    def seen(base):
        return (base <= query_base + tokens - 1) & (base + tokens - 1 >= earliest)

    def needed(i):
        return seen(bases[i])

    group = QUERY_HEAD_COUNT // KEY_VALUE_HEADS
    pairs = group // PAIR
    steps = [(g, layer, pair) for g in range(KEY_VALUE_HEADS) for layer in range(2) for pair in range(pairs)]
    factor = math.log2(math.e) / math.sqrt(HEAD_WIDTH)

    def scores(step, active):
        g, layer, pair = step
        source = (first_ref, second_ref)[layer]
        head = g * group + pair * PAIR
        query = jnp.concatenate(
            [source[:, (head + i) * HEAD_WIDTH : (head + i + 1) * HEAD_WIDTH] for i in range(PAIR)], axis=0
        )
        keys = jnp.concatenate([blocks[i][g] for i in active], axis=0)
        return lax.dot_general(keys, query, (((1,), (1,)), ((), ())), preferred_element_type=jnp.float32)

    def weigh(n, raw):
        masked = raw * factor + bias_ref[: raw.shape[0], :]
        highest = jnp.max(masked, axis=0, keepdims=True)
        fade = None
        if not first:
            former = stat_in[2 * n : 2 * n + 1, :]
            highest = jnp.maximum(highest, former)
            fade = jnp.exp2(former - highest)
        weights = jnp.exp2(masked - highest)
        return n, weights.astype(jnp.bfloat16), highest, fade

    def gather(active, n, rounded, highest, fade):
        values = jnp.concatenate([blocks[i][KEY_VALUE_HEADS + steps[n][0]] for i in active], axis=1)
        values = jnp.concatenate([values, jnp.ones((ONES, values.shape[1]), values.dtype)], axis=0)
        product = jnp.dot(values, rounded, preferred_element_type=jnp.float32)
        product, row_sum = product[:HEAD_WIDTH], product[HEAD_WIDTH : HEAD_WIDTH + 1]
        if not first:
            row_sum = row_sum + stat_in[2 * n + 1 : 2 * n + 2, :] * fade
            product = product + sum_in[n] * fade
        finish(n, steps[n], product, row_sum, highest)

    def absorb(active):
        place = query_base + lax.broadcasted_iota(jnp.int32, (1, tokens), 1)
        start = start_of(place)
        for row, i in enumerate(active):
            key_place = bases[i] + lax.broadcasted_iota(jnp.int32, (tokens, tokens), 0)
            visible = (key_place >= start) & (key_place <= place)
            bias = jnp.where(visible, 0.0, HIDDEN)
            for j in range(PAIR):
                bias_ref[row * tokens : (row + 1) * tokens, j * tokens : (j + 1) * tokens] = bias

        ahead = 1 if len(active) > 2 else 3
        early = [scores(step, active) for step in steps[:ahead]]
        late = []
        for n in range(len(steps)):
            if n + ahead < len(steps):
                early.append(scores(steps[n + ahead], active))
            if len(late) > BEHIND:
                gather(active, *late.pop(0))
            late.append(weigh(n, early.pop(0)))
        for item in late:
            gather(active, *item)

    def leaving(n):
        g, layer, pair = steps[n]
        columns = pl.ds((g * group + pair * PAIR) * HEAD_WIDTH, PAIR * HEAD_WIDTH)
        return pltpu.make_async_copy(out_refs[layer].at[:, columns], gone_refs[layer].at[:, columns], left.at[n])

    def settle(n, step, product, row_sum):
            g, layer, pair = step
            blended = (product * (1.0 / row_sum)).astype(jnp.bfloat16)
            head = g * group + pair * PAIR
            for i in range(PAIR):
                columns = slice((head + i) * HEAD_WIDTH, (head + i + 1) * HEAD_WIDTH)
                out_refs[layer][:, columns] = blended[:, i * tokens : (i + 1) * tokens].T
            leaving(n).start()

    def depart():
        for n in range(len(steps)):
            leaving(n).wait()

    def finish(n, step, product, row_sum, highest):
        if last:
            settle(n, step, product, row_sum)
        else:
            sum_ref[n] = product
            stat_ref[2 * n : 2 * n + 1, :] = highest
            stat_ref[2 * n + 1 : 2 * n + 2, :] = row_sum

    if first:
        both = needed(1)
        pl.when(both)(lambda: absorb([0, 1]))
        pl.when(jnp.logical_not(both))(lambda: absorb([0]))
        return

    near = needed(0) | needed(1)
    if last:

        @pl.when(near)
        def _():
            absorb([0, 1])
            depart()

        return

    far = needed(count - 2) | needed(count - 1)
    pl.when(near & far)(lambda: absorb(list(range(count))))
    pl.when(near & jnp.logical_not(far))(lambda: absorb([0, 1]))
    pl.when(far & jnp.logical_not(near))(lambda: absorb([count - 2, count - 1]))

    kept = jnp.logical_not(near | far)
    if later:
        awaited = functools.reduce(jnp.logical_or, [seen(source(device) * tokens) for source in later])

        @pl.when(jnp.logical_not(kept | awaited))
        def _():
            for n, step in enumerate(steps):
                settle(n, step, sum_ref[n], stat_ref[2 * n + 1 : 2 * n + 2, :])
            depart()

        @pl.when(kept & jnp.logical_not(awaited))
        def _():
            for n, step in enumerate(steps):
                settle(n, step, sum_in[n], stat_in[2 * n + 1 : 2 * n + 2, :])
            depart()

        kept = kept & awaited

    @pl.when(kept)
    def _():
        for n, step in enumerate(steps):
            finish(n, step, sum_in[n], stat_in[2 * n + 1 : 2 * n + 2, :], stat_in[2 * n : 2 * n + 1, :])


def attend(device, lengths, first_queries, second_queries, blocks, sources, state, later=(), outputs=()):
    tokens = first_queries.shape[0]
    steps = 2 * QUERY_HEAD_COUNT // PAIR
    width = PAIR * tokens
    state_shapes = [
        jax.ShapeDtypeStruct((steps, HEAD_WIDTH, width), jnp.float32),
        jax.ShapeDtypeStruct((2 * steps, width), jnp.float32),
    ]
    in_vmem = pl.BlockSpec(memory_space=pltpu.VMEM)
    in_smem = pl.BlockSpec(memory_space=pltpu.SMEM)
    first = state is None
    last = bool(outputs)
    in_hbm = pl.BlockSpec(memory_space=pltpu.HBM)
    operands = [device, lengths, first_queries, second_queries, *blocks]
    aliases = {}
    if not first:
        if not last:
            aliases = {len(operands): 0, len(operands) + 1: 1}
        operands += state
    if last:
        aliases = {len(operands): 0, len(operands) + 1: 1}
        operands += outputs
    keys = len(blocks) * tokens
    outs = [jax.ShapeDtypeStruct(q.shape, q.dtype) for q in (first_queries, second_queries)]
    if not last:
        outs = state_shapes + (outs if later else [])
    leaving = [pltpu.VMEM(q.shape, q.dtype) for q in (first_queries, second_queries)]
    leaving.append(pltpu.SemaphoreType.DMA((steps,)))
    return pl.pallas_call(
        functools.partial(attend_kernel, sources, later, len(blocks), first, last),
        out_shape=outs,
        in_specs=[in_smem, in_smem] + [in_vmem] * (len(operands) - 2 - len(outputs)) + [in_hbm] * len(outputs),
        out_specs=[in_hbm] * 2 if last else [in_vmem] * 2 + [in_hbm] * (len(outs) - 2),
        scratch_shapes=[
            *(leaving if last or later else []),
            pltpu.VMEM((keys, width), jnp.float32),
        ],
        input_output_aliases=aliases,
        cost_estimate=pl.CostEstimate(
            flops=steps * 4 * keys * width * HEAD_WIDTH,
            bytes_accessed=2 * first_queries.size * 2 + 2 * keys * 2 * KEY_VALUE_HEADS * HEAD_WIDTH,
            transcendentals=steps * keys * width,
        ),
        compiler_params=pltpu.CompilerParams(vmem_limit_bytes=GRANT),
        name="attend_last" if last else "attend",
    )(*operands)


def on_device(first_queries, second_queries, common_keys, common_values, lengths):
    members = lax.axis_size("seq")
    rounds = members // 2 // LEVEL
    device = lax.axis_index("seq").astype(jnp.int32).reshape(1)

    def send(block, route):
        return lax.ppermute(block, "seq", route)

    def core(block):
        return send(block, swapped(members, CORE))

    def row(block):
        return send(block, swapped(members, ROW))

    def behind(levels, flip):
        return lambda d: (d ^ flip) - levels * LEVEL

    def upper_behind(levels, flip):
        return lambda d: jnp.where(d & ROW == 0, (d ^ flip) - levels * LEVEL, NOWHERE)

    own = pack(common_keys, common_values)
    step = functools.partial(attend, device, lengths, first_queries, second_queries)
    previous = send(own, shifted(members))
    beside = row(own)
    partner = core(own)
    state = step([own, partner], [behind(0, 0), behind(0, CORE)], None)

    blocks, sources = [beside, core(beside)], [behind(0, ROW), behind(0, ROW | CORE)]
    for level in range(1, rounds):
        blocks += [previous, core(previous)]
        sources += [behind(level, 0), behind(level, CORE)]
        following = send(previous, shifted(members))
        over = row(previous)
        if level == rounds - 1:
            corner = send(previous, across(members, level))
        state = step(blocks, sources, state)
        blocks, sources = [over, core(over)], [behind(level, ROW), behind(level, ROW | CORE)]
        previous = following
    blocks += [previous, core(previous)]
    sources += [behind(rounds, 0), behind(rounds, CORE)]
    later = [upper_behind(rounds, ROW), upper_behind(rounds, ROW | CORE)]
    *state, first_output, second_output = step(blocks, sources, state, later)
    blocks = [corner, core(corner)]
    return tuple(step(blocks, later, state, outputs=[first_output, second_output]))


def solution(mesh):
    tokens = P(("groups", "seq"), None)
    return jax.shard_map(
        on_device,
        mesh=mesh,
        in_specs=(tokens, tokens, tokens, tokens, P("groups")),
        out_specs=(tokens, tokens),
        check_vma=False,
    )
```
